32 devices in a mesh: gx: 2 (over y), gy: 4 (over z), gz: 4 (over x, core).
Axes of the slice: x: 2, y: 2, z: 4, core: 2. Of those that a mesh axis runs over, the one named last changes fastest.
Arguments:
- positions: float32 [2, 4, 4, 3, 48], P('gx', 'gy', 'gz'), may hold values from 0 to 1
- species: int32 [2, 4, 4, 48], P('gx', 'gy', 'gz'), may hold values from 0 to 3
- neighbours: int32 [2, 4, 4, 48, 128], P('gx', 'gy', 'gz'), may hold values from 0 to 1295
- neigh_counts: int32 [2, 4, 4, 48], P('gx', 'gy', 'gz'), may hold values from 64 to 128
- embedding: bfloat16 [4, 128], replicated, may hold values from -6 to 6
- rbf_decay: float32 [16], replicated, may hold values from 0.2 to 5
- radial_weight: bfloat16 [2, 16, 128], replicated, may hold values from -1.5 to 1.5
- node_weight: bfloat16 [2, 128, 128], replicated, may hold values from -0.5 to 0.5
- readout: bfloat16 [128], replicated, may hold values from -0.5 to 0.5
- species_bias: float32 [4], replicated, may hold values from -4 to 4
Outputs:
- atom_energy: float32 [2, 4, 4, 48], P('gx', 'gy', 'gz')
- total_energy: float32 [], replicated
The draws below stay inside these ranges and needn't reach their ends.
Inputs may be any that keep to these rules, and one draw needn't show every extreme that they name: `neighbours`: the offset code of an entry is 9 (dx + 1) + 3 (dy + 1) + (dz + 1) for a cell offset of -1, 0 or 1 along each dimension.
All inputs are finite; a program needn't handle non-finite values.
Results may differ from the reference program's by a relative error of at most 0.0028.
Values may be sent and summed in bfloat16 or wider, within the bound.
A program may use at most 64 MiB of HBM per device.

```python
import math
import jax
import jax.numpy as jnp
from jax import lax

F = 128
NB = 128
NRBF = 16
NSPEC = 4
SLOTS = 48
LAYERS = 2
NX = 2
NY = 4
NZ = 4


def plant(result, key, least, largest):
    extent = result.shape
    spot = [jax.random.randint(jax.random.fold_in(key, axis), (), 0, extent[axis]) for axis in range(len(extent))]
    result = result.at[tuple(spot)].set(least)
    longest = extent.index(max(extent))
    spot[longest] = (spot[longest] + 1) % extent[longest]
    return result.at[tuple(spot)].set(largest)


def block_levels(rng, shape, cuts, smallest, top_value):
    loudness = 1.0
    for dim, blocks in cuts:
        draws = jax.random.uniform(jax.random.fold_in(jax.random.fold_in(rng, 6), dim), (blocks,), jnp.float32, smallest / len(cuts), top_value / len(cuts))
        loudness = loudness * jnp.repeat(jnp.exp(draws), shape[dim] // blocks).reshape((-1,) + (1,) * (len(shape) - 1 - dim))
    return loudness


def bell_draw(stream_key, shape, spread, most, kind=jnp.bfloat16):
    entries = spread * jax.random.normal(stream_key, shape, jnp.float32)
    return jnp.clip(entries, min=-most, max=most).astype(kind)


def setup_inputs(seed: int = 0) -> dict:
    splits = jax.random.split(jax.random.key(seed), 11)
    return {
        "positions": jnp.clip(1.0 * jax.random.uniform(splits[0], (NX, NY, NZ, 3, SLOTS), jnp.float32) ** block_levels(splits[0], (NX, NY, NZ, 3, SLOTS), ((0, 2), (1, 4), (2, 4)), -0.2, 0.2), 0.0, 1.0),
        "species": plant(jax.random.randint(splits[1], (NX, NY, NZ, SLOTS), 0, NSPEC), jax.random.fold_in(splits[1], 1), 0, NSPEC - 1).astype(jnp.int32),
        "neighbours": plant(jax.random.randint(splits[2], (NX, NY, NZ, SLOTS, NB), 0, 27 * SLOTS), jax.random.fold_in(splits[2], 1), 0, (27 * SLOTS) - 1).astype(jnp.int32),
        "neigh_counts": plant(jax.random.randint(splits[3], (NX, NY, NZ, SLOTS), NB // 2, NB + 1), jax.random.fold_in(splits[3], 1), NB // 2, NB).astype(jnp.int32),
        "embedding": bell_draw(splits[4], (NSPEC, F), 1.0, 6.0),
        "rbf_decay": jnp.clip(jnp.exp(jax.random.uniform(splits[5], (NRBF,), jnp.float32, math.log(0.2), math.log(5.0))), 0.2, 5.0),
        "radial_weight": bell_draw(splits[6], (LAYERS, NRBF, F), NRBF ** -0.5, 1.5),
        "node_weight": bell_draw(splits[7], (LAYERS, F, F), F ** -0.5, 0.5),
        "readout": bell_draw(splits[8], (F,), F ** -0.5, 0.5),
        "species_bias": bell_draw(splits[9], (NSPEC,), 1.0, 4.0, jnp.float32),
    }


def embed_atoms(species, embedding):
    kind_count = embedding.shape[0]
    one_hot = (species[..., None] == jnp.arange(kind_count, dtype=jnp.int32)).astype(jnp.bfloat16)
    embedded = jnp.dot(one_hot.reshape(-1, kind_count), embedding, preferred_element_type=jnp.float32)
    return embedded.astype(jnp.bfloat16).reshape(species.shape + (embedding.shape[1],))

def interaction(hidden_slab, place_slab, neighbour_row, count_row, rbf_decay, radial_weight, node_weight):
    cell_count, slot_count, neighbour_count = neighbour_row.shape
    feature_width = hidden_slab.shape[-1]
    slab_depth = cell_count + 2
    code_offset = neighbour_row // slot_count
    slot_index = neighbour_row % slot_count
    shift_x = code_offset // 9
    shift_y = code_offset // 3 % 3
    shift_z = code_offset % 3
    cell_column = lax.broadcasted_iota(jnp.int32, neighbour_row.shape, 0)
    cell_index = ((shift_x * 3 + shift_y) * slab_depth + cell_column + shift_z).reshape(-1)
    slot_flat = slot_index.reshape(-1)
    neighbour_feats = jnp.take(hidden_slab.reshape(-1, feature_width), cell_index * slot_count + slot_flat, axis=0)
    place_flat = place_slab.reshape(9 * slab_depth, 3, slot_count)
    far_place = place_flat[cell_index, :, slot_flat]
    centre = jnp.transpose(place_slab[1, 1, 1:slab_depth - 1], (0, 2, 1))
    offsets_xyz = jnp.stack([shift_x - 1, shift_y - 1, shift_z - 1], axis=-1).astype(jnp.float32)
    displace = far_place.reshape(cell_count, slot_count, neighbour_count, 3) + offsets_xyz - centre[:, :, None, :]
    distance_sq = lax.optimization_barrier(jnp.sum(displace * displace, axis=-1))
    radial_basis = jnp.exp(-distance_sq[..., None] * rbf_decay).astype(jnp.bfloat16).reshape(-1, rbf_decay.shape[0])
    filters = jnp.dot(radial_basis, radial_weight, preferred_element_type=jnp.float32)
    live_mask = (lax.broadcasted_iota(jnp.int32, neighbour_row.shape, 2) < count_row[:, :, None]).reshape(-1, 1)
    terms = jnp.where(live_mask, filters * neighbour_feats.astype(jnp.float32), jnp.float32(0.0))
    message = terms.reshape(cell_count * slot_count, neighbour_count, feature_width).sum(axis=1)
    inv_scale = lax.rsqrt(lax.optimization_barrier(jnp.mean(message * message, axis=-1, keepdims=True)) + 1e-05)
    normed = (message * inv_scale).astype(jnp.bfloat16)
    update = jax.nn.silu(jnp.dot(normed, node_weight, preferred_element_type=jnp.float32))
    own_rows = hidden_slab[1, 1, 1:slab_depth - 1].reshape(-1, feature_width).astype(jnp.float32)
    return (own_rows + update).astype(jnp.bfloat16).reshape(cell_count, slot_count, feature_width)

def run_layer(hidden_pad, place_pad, neighbours, neigh_counts, rbf_decay, radial_weight, node_weight):
    span_x = neighbours.shape[0]
    span_y = neighbours.shape[1]

    def one_row(row_index):
        row_x = row_index // span_y
        row_y = row_index % span_y
        hidden_slab = lax.dynamic_slice_in_dim(lax.dynamic_slice_in_dim(hidden_pad, row_x, 3, 0), row_y, 3, 1)
        place_slab = lax.dynamic_slice_in_dim(lax.dynamic_slice_in_dim(place_pad, row_x, 3, 0), row_y, 3, 1)
        return interaction(hidden_slab, place_slab, neighbours[row_x, row_y], neigh_counts[row_x, row_y], rbf_decay, radial_weight, node_weight)
    row_results = lax.map(one_row, jnp.arange(span_x * span_y, dtype=jnp.int32))
    return row_results.reshape((span_x, span_y) + row_results.shape[1:])

def atom_energies(hidden, species, readout, species_bias):
    per_atom = lax.optimization_barrier(jnp.sum(hidden.astype(jnp.float32) * readout.astype(jnp.float32), axis=-1))
    one_hot = (species[..., None] == jnp.arange(species_bias.shape[0], dtype=jnp.int32)).astype(jnp.float32)
    return per_atom + lax.optimization_barrier(jnp.sum(one_hot * species_bias, axis=-1))

def reference(positions, species, neighbours, neigh_counts, embedding, rbf_decay, radial_weight, node_weight, readout, species_bias):
    pad_spec = ((1, 1), (1, 1), (1, 1), (0, 0), (0, 0))
    place_pad = jnp.pad(positions, pad_spec, mode='wrap')
    hidden = embed_atoms(species, embedding)
    for layer_index in range(LAYERS):
        hidden_pad = jnp.pad(hidden, pad_spec, mode='wrap')
        hidden = run_layer(hidden_pad, place_pad, neighbours, neigh_counts, rbf_decay, radial_weight[layer_index], node_weight[layer_index])
    energy = atom_energies(hidden, species, readout, species_bias)
    return (energy, jnp.sum(energy))
```

```python
import functools
import itertools
import math

import jax
import jax.numpy as jnp
from jax import lax
from jax.experimental import pallas as pl
from jax.experimental.pallas import tpu as pltpu
from jax.sharding import PartitionSpec as P

AXES = ("gx", "gy", "gz")
MESH = pl.DeviceIdType.MESH
LANES = 128
LOG2E = math.log2(math.e)


def distinct(count):
    return (0,) if count == 1 else (0, -1) if count == 2 else (0, -1, 1)


def canonical(offset, count):
    return 0 if count == 1 else -abs(offset) if count == 2 else offset


def code_of(offset):
    return 9 * (offset[0] + 1) + 3 * (offset[1] + 1) + offset[2] + 1


def kernel(
    sizes,
    stages,
    pos_ref,
    spec_ref,
    nbr_ref,
    cnt_ref,
    emb_ref,
    decay_ref,
    radial_ref,
    node_ref,
    readout_ref,
    bias_ref,
    energy_ref,
    total_ref,
    record,
    places,
    hist,
    codes,
    basis,
    feats0,
    feats1,
    *rest,
):
    stage_bufs = rest[: len(stages)]
    pos_send, pos_recv, hid_send, hid_recv = rest[len(stages) : len(stages) + 4]
    stage_sems = rest[len(stages) + 4 :]
    me = tuple(lax.axis_index(name) for name in AXES)
    slots = pos_ref.shape[-1]
    neighbour_count = nbr_ref.shape[-1]
    features = emb_ref.shape[1]
    kinds = emb_ref.shape[0]
    basis_count = radial_ref.shape[1]
    layers = radial_ref.shape[0]
    tiles = basis.shape[1] // LANES
    hi_rows = hist.shape[0] // slots

    def device(shift):
        return tuple(
            lax.rem(coord + (delta % count), count) if delta % count else coord
            for coord, delta, count in zip(me, shift, sizes)
        )

    neighbours = [
        off for off in itertools.product(*(distinct(n) for n in sizes)) if off != (0, 0, 0)
    ]
    stage_shifts = [
        [
            shift
            for shift in itertools.product(
                *(range(n) if name in axes else (0,) for name, n in zip(AXES, sizes))
            )
            if any(shift)
        ]
        for axes in stages
    ]
    partners = {tuple((-d) % n for d, n in zip(off, sizes)) for off in neighbours}
    for shifts in stage_shifts:
        partners.update(shifts)
    barrier = pltpu.get_barrier_semaphore()
    for shift in sorted(partners):
        pl.semaphore_signal(barrier, inc=1, device_id=device(shift), device_id_type=MESH)

    record[...] = jnp.zeros(record.shape, jnp.float32)
    record[0:3, 0:slots] = pos_ref[0, 0, 0]
    record[3:4, 0:slots] = spec_ref[0, 0].astype(jnp.float32)
    record[4:5, 0:slots] = cnt_ref[0, 0].astype(jnp.float32)
    columns = jnp.transpose(record[...])[0:slots]
    own_pos = [
        jnp.broadcast_to(columns[:, c : c + 1], (slots, LANES)) for c in range(3)
    ]
    species_col = columns[:, 3:4]
    count_col = columns[:, 4:5]

    pl.semaphore_wait(barrier, len(partners))

    def place_copy(off):
        code = code_of(off)
        return pltpu.make_async_remote_copy(
            src_ref=record,
            dst_ref=places.at[code],
            send_sem=pos_send.at[code],
            recv_sem=pos_recv.at[code],
            device_id=device(tuple(-d for d in off)),
            device_id_type=MESH,
        )

    place_copies = [place_copy(off) for off in neighbours]
    for copy in place_copies:
        copy.start()

    raw = nbr_ref[0, 0, 0]
    live = lax.broadcasted_iota(jnp.int32, raw.shape, 1).astype(jnp.float32) < count_col
    codes[...] = jnp.where(live, raw, hi_rows * LANES - 1)
    hi_iota = lax.broadcasted_iota(jnp.int32, (hi_rows, neighbour_count), 0)
    lo_iota = lax.broadcasted_iota(jnp.int32, (LANES, neighbour_count), 0)
    for atom in range(slots):
        row = codes[atom : atom + 1, :]
        high = jnp.where((row >> 7) == hi_iota, 1.0, 0.0).astype(jnp.bfloat16)
        low = jnp.where((row & (LANES - 1)) == lo_iota, 1.0, 0.0).astype(jnp.bfloat16)
        hist[atom * hi_rows : (atom + 1) * hi_rows, :] = lax.dot_general(
            high, low, (((1,), (1,)), ((), ())), preferred_element_type=jnp.float32
        )

    own_hidden = jnp.zeros((slots, features), jnp.float32)
    for kind in range(kinds):
        own_hidden = jnp.where(
            species_col == float(kind), emb_ref[kind : kind + 1, :].astype(jnp.float32), own_hidden
        )
    table_rows = feats1.shape[0]
    feats1[27 * slots : table_rows, :] = jnp.zeros(
        (table_rows - 27 * slots, features), jnp.bfloat16
    )
    emb = emb_ref[...].astype(jnp.float32)
    if kinds < 8:
        emb = jnp.concatenate([emb, jnp.zeros((8 - kinds, features), jnp.float32)], axis=0)
    emb = emb.astype(jnp.bfloat16)
    scales = [decay_ref[b] * (-LOG2E) for b in range(basis_count)]

    lane = lax.broadcasted_iota(jnp.int32, (8, LANES), 1)
    sub = lax.broadcasted_iota(jnp.int32, (8, LANES), 0)
    for copy in place_copies:
        copy.wait_recv()

    flat = [jnp.zeros((8, LANES), jnp.float32) for _ in range(tiles)]
    for off in itertools.product((-1, 0, 1), repeat=3):
        source = tuple(canonical(d, n) for d, n in zip(off, sizes))
        cell = record[...] if source == (0, 0, 0) else places[code_of(source)]
        for component, delta in enumerate(off):
            if delta:
                cell = jnp.where(sub == component, cell + float(delta), cell)
        tile, start = divmod(code_of(off) * slots, LANES)
        if start:
            cell = pltpu.roll(cell, start, 1)
        stop = start + slots
        flat[tile] = jnp.where((lane >= start) & (lane < stop), cell, flat[tile])
        if stop > LANES:
            flat[tile + 1] = jnp.where(lane < stop - LANES, cell, flat[tile + 1])

    for tile in range(tiles):
        span = slice(tile * LANES, (tile + 1) * LANES)
        r2 = jnp.zeros((slots, LANES), jnp.float32)
        for c in range(3):
            delta = flat[tile][c : c + 1, :] - own_pos[c]
            r2 = r2 + delta * delta
        times = hist[pl.ds(tile, slots, stride=hi_rows), :]
        for b in range(basis_count):
            basis[b * slots : (b + 1) * slots, span] = (
                jnp.exp2(r2 * scales[b]) * times
            ).astype(jnp.bfloat16)
        one_hot = jnp.where(
            flat[tile][3:4, :].astype(jnp.int32) == sub, 1.0, 0.0
        )
        feats0[span, :] = jnp.dot(
            jnp.transpose(one_hot).astype(jnp.bfloat16), emb, preferred_element_type=jnp.float32
        ).astype(jnp.bfloat16)

    def interaction(layer, feats, hidden):
        collected = jnp.dot(basis[...], feats[...], preferred_element_type=jnp.float32)
        weight = radial_ref[layer].astype(jnp.float32)
        message = jnp.zeros((slots, features), jnp.float32)
        for b in range(basis_count):
            message = message + collected[b * slots : (b + 1) * slots] * weight[b : b + 1]
        inv_scale = lax.rsqrt(jnp.mean(message * message, axis=-1, keepdims=True) + 1e-05)
        normed = (message * inv_scale).astype(jnp.bfloat16)
        value = jnp.dot(normed, node_ref[layer], preferred_element_type=jnp.float32)
        update = value / (1.0 + jnp.exp(-value))
        return (hidden + update).astype(jnp.bfloat16)

    hidden1 = interaction(0, feats0, own_hidden)
    own_rows = pl.ds(code_of((0, 0, 0)) * slots, slots)
    feats1[own_rows, :] = hidden1

    def hidden_copy(off):
        code = code_of(off)
        return pltpu.make_async_remote_copy(
            src_ref=feats1.at[own_rows],
            dst_ref=feats1.at[pl.ds(code * slots, slots)],
            send_sem=hid_send.at[code],
            recv_sem=hid_recv.at[code],
            device_id=device(tuple(-d for d in off)),
            device_id_type=MESH,
        )

    hidden_copies = [hidden_copy(off) for off in neighbours]
    for copy in hidden_copies:
        copy.start()

    species_row = record[3:4, :]
    offsets = jnp.zeros((1, LANES), jnp.float32)
    for kind in range(kinds):
        offsets = jnp.where(species_row == float(kind), bias_ref[kind], offsets)
    offsets = jnp.where(lane[0:1] < slots, offsets, 0.0)

    for copy in hidden_copies:
        copy.wait_recv()
    for off in itertools.product((-1, 0, 1), repeat=3):
        source = tuple(canonical(d, n) for d, n in zip(off, sizes))
        if source != off:
            feats1[pl.ds(code_of(off) * slots, slots), :] = feats1[
                pl.ds(code_of(source) * slots, slots), :
            ]
    hidden2 = interaction(1, feats1, hidden1.astype(jnp.float32))
    padded = jnp.concatenate(
        [hidden2, jnp.zeros((LANES - slots, features), jnp.bfloat16)], axis=0
    )
    readout = jnp.broadcast_to(readout_ref[...], (16, features))
    per_atom = lax.dot_general(
        readout, padded, (((1,), (1,)), ((), ())), preferred_element_type=jnp.float32
    )
    running = per_atom[0:1, :] + offsets
    energy_ref[0, 0] = running[:, 0:slots]

    for axes, shifts, buf, send, recv in zip(
        stages, stage_shifts, stage_bufs, stage_sems[0::2], stage_sems[1::2]
    ):
        def rank_of(coords):
            rank = 0
            for name, coord, count in zip(AXES, coords, sizes):
                if name in axes:
                    rank = rank * count + coord
            return rank

        mine = rank_of(me)
        buf[mine] = running
        copies = []
        for index, shift in enumerate(shifts):
            copies.append(
                pltpu.make_async_remote_copy(
                    src_ref=buf.at[mine],
                    dst_ref=buf.at[mine],
                    send_sem=send.at[index],
                    recv_sem=recv.at[index],
                    device_id=device(shift),
                    device_id_type=MESH,
                )
            )
        for copy in copies:
            copy.start()
        for copy in copies:
            copy.wait_recv()
        running = jnp.sum(buf[...], axis=0)
        for copy in copies:
            copy.wait_send()
    total_ref[...] = jnp.sum(running, axis=1, keepdims=True)
    for copy in place_copies + hidden_copies:
        copy.wait_send()


def body(sizes, *args):
    positions, species, neighbours, _, embedding, decay, radial, _, readout, _ = args
    slots = positions.shape[-1]
    features = embedding.shape[1]
    basis_count = decay.shape[0]
    tiles = pl.cdiv(27 * slots, LANES)
    hi_rows = 16 * pl.cdiv(tiles + 1, 16)
    devices = math.prod(sizes)
    stages = (AXES,) if devices <= 64 else tuple((name,) for name in AXES)
    stage_ranks = [
        math.prod(n for name, n in zip(AXES, sizes) if name in axes) for axes in stages
    ]
    vmem = pl.BlockSpec(memory_space=pltpu.VMEM)
    smem = pl.BlockSpec(memory_space=pltpu.SMEM)
    dma = pltpu.SemaphoreType.DMA
    scratch = [
        pltpu.VMEM((8, LANES), jnp.float32),
        pltpu.VMEM((27, 8, LANES), jnp.float32),
        pltpu.VMEM((slots * hi_rows, LANES), jnp.float32),
        pltpu.VMEM((slots, neighbours.shape[-1]), jnp.int32),
        pltpu.VMEM((basis_count * slots, tiles * LANES), jnp.bfloat16),
        pltpu.VMEM((tiles * LANES, features), jnp.bfloat16),
        pltpu.VMEM((tiles * LANES, features), jnp.bfloat16),
    ]
    scratch += [pltpu.VMEM((count, 1, LANES), jnp.float32) for count in stage_ranks]
    scratch += [dma((27,))] * 4
    for count in stage_ranks:
        scratch += [dma((max(count - 1, 1),))] * 2
    energy, total = pl.pallas_call(
        functools.partial(kernel, sizes, stages),
        out_shape=(
            jax.ShapeDtypeStruct(species.shape, jnp.float32),
            jax.ShapeDtypeStruct((1, 1), jnp.float32),
        ),
        in_specs=[vmem, vmem, vmem, vmem, vmem, smem, vmem, vmem, vmem, smem],
        out_specs=(vmem, vmem),
        scratch_shapes=scratch,
        compiler_params=pltpu.CompilerParams(collective_id=0, has_side_effects=True),
    )(*args[:8], readout.reshape(1, features), args[9])
    return energy, total.reshape(())


def solution(mesh):
    sizes = tuple(mesh.shape[name] for name in AXES)
    return jax.shard_map(
        functools.partial(body, sizes),
        mesh=mesh,
        in_specs=(
            P("gx", "gy", "gz", None, None),
            P("gx", "gy", "gz", None),
            P("gx", "gy", "gz", None, None),
            P("gx", "gy", "gz", None),
            P(),
            P(),
            P(),
            P(),
            P(),
            P(),
        ),
        out_specs=(P("gx", "gy", "gz", None), P()),
        check_vma=False,
    )
```

```python
import functools
import itertools
import math

import jax
import jax.numpy as jnp
from jax import lax
from jax.experimental import pallas as pl
from jax.experimental.pallas import tpu as pltpu
from jax.sharding import PartitionSpec as P

AXES = ("gx", "gy", "gz")
MESH = pl.DeviceIdType.MESH
LANES = 128
LOG2E = math.log2(math.e)


def distinct(count):
    return (0,) if count == 1 else (0, -1) if count == 2 else (0, -1, 1)


def canonical(offset, count):
    return 0 if count == 1 else -abs(offset) if count == 2 else offset


def code_of(offset):
    return 9 * (offset[0] + 1) + 3 * (offset[1] + 1) + offset[2] + 1


def fold_of(sizes, slots):
    merge = sizes[0] == 2
    lead = 18 * slots
    shift = -lead % LANES if merge else 0
    return merge, lead, shift, pl.cdiv(27 * slots + shift, LANES)


def kernel(
    sizes,
    stages,
    pos_any,
    spec_any,
    nbr_any,
    cnt_any,
    emb_any,
    decay_any,
    radial_any,
    node_any,
    readout_any,
    bias_any,
    out_ref,
    record,
    places,
    hist,
    codes,
    basis,
    feats0,
    feats1,
    *rest,
):
    anys = (
        pos_any, spec_any, nbr_any, cnt_any, emb_any, decay_any, radial_any, node_any, readout_any, bias_any,
    )
    pos_ref, spec_ref, nbr_ref, cnt_ref, emb_ref = rest[:5]
    decay_ref, radial_ref, node_ref, readout_ref, bias_ref = rest[5:10]
    load_sem = rest[10]
    loads = [
        pltpu.make_async_copy(src, dst, load_sem.at[n])
        for n, (src, dst) in enumerate(zip(anys, rest[:10]))
    ]
    rest = rest[11:]
    stage_bufs = rest[: len(stages)]
    pos_send, pos_recv, hid_send, hid_recv = rest[len(stages) : len(stages) + 4]
    stage_sems = rest[len(stages) + 4 :]
    me = tuple(lax.axis_index(name) for name in AXES)
    slots = pos_any.shape[-1]
    neighbour_count = nbr_any.shape[-1]
    features = emb_any.shape[1]
    kinds = emb_any.shape[0]
    basis_count = radial_ref.shape[1]
    layers = radial_ref.shape[0]
    tiles = basis.shape[1] // LANES
    merge, lead, shift_x, tables = fold_of(sizes, slots)
    first = (lead + shift_x) // LANES
    kept = lead if merge else 27 * slots
    hi_rows = hist.shape[0] // slots

    def device(shift):
        return tuple(
            lax.rem(coord + (delta % count), count) if delta % count else coord
            for coord, delta, count in zip(me, shift, sizes)
        )

    neighbours = [
        off for off in itertools.product(*(distinct(n) for n in sizes)) if off != (0, 0, 0)
    ]
    stage_shifts = [
        [
            shift
            for shift in itertools.product(
                *(range(n) if name in axes else (0,) for name, n in zip(AXES, sizes))
            )
            if any(shift)
        ]
        for axes in stages
    ]
    partners = {tuple((-d) % n for d, n in zip(off, sizes)) for off in neighbours}
    for shifts in stage_shifts:
        partners.update(shifts)
    barrier = pltpu.get_barrier_semaphore()
    for shift in sorted(partners):
        pl.semaphore_signal(barrier, inc=1, device_id=device(shift), device_id_type=MESH)

    for n in (0, 1, 3, 2, 4, 5, 6, 7, 8, 9):
        loads[n].start()
    for n in (0, 1, 3):
        loads[n].wait()
    record[...] = jnp.zeros(record.shape, jnp.float32)
    record[0:3, 0:slots] = pos_ref[0, 0, :, 0]
    record[3:4, 0:slots] = spec_ref[0, 0].astype(jnp.float32)
    record[4:5, 0:slots] = cnt_ref[0, 0].astype(jnp.float32)
    columns = jnp.transpose(record[...])[0:slots]
    own_pos = [
        jnp.broadcast_to(columns[:, c : c + 1], (slots, LANES)) for c in range(3)
    ]
    species_col = columns[:, 3:4]
    count_col = columns[:, 4:5]

    pl.semaphore_wait(barrier, len(partners))

    def place_copy(off):
        code = code_of(off)
        return pltpu.make_async_remote_copy(
            src_ref=record,
            dst_ref=places.at[code],
            send_sem=pos_send.at[code],
            recv_sem=pos_recv.at[code],
            device_id=device(tuple(-d for d in off)),
            device_id_type=MESH,
        )

    place_copies = [place_copy(off) for off in neighbours]
    for copy in place_copies:
        copy.start()

    loads[2].wait()
    raw = nbr_ref[0, 0, 0]
    live = lax.broadcasted_iota(jnp.int32, raw.shape, 1).astype(jnp.float32) < count_col
    raw = jnp.where(raw >= lead, raw + shift_x, raw)
    codes[...] = jnp.where(live, raw, hi_rows * LANES - 1)
    hi_iota = lax.broadcasted_iota(jnp.int32, (hi_rows, neighbour_count), 0)
    lo_iota = lax.broadcasted_iota(jnp.int32, (LANES, neighbour_count), 0)
    for atom in range(slots):
        row = codes[atom : atom + 1, :]
        high = jnp.where((row >> 7) == hi_iota, 1.0, 0.0).astype(jnp.bfloat16)
        low = jnp.where((row & (LANES - 1)) == lo_iota, 1.0, 0.0).astype(jnp.bfloat16)
        hist[atom * hi_rows : (atom + 1) * hi_rows, :] = lax.dot_general(
            high, low, (((1,), (1,)), ((), ())), preferred_element_type=jnp.float32
        )

    for n in range(4, 10):
        loads[n].wait()
    own_hidden = jnp.zeros((slots, features), jnp.float32)
    for kind in range(kinds):
        own_hidden = jnp.where(
            species_col == float(kind), emb_ref[kind : kind + 1, :].astype(jnp.float32), own_hidden
        )
    table_rows = feats1.shape[0]
    if table_rows > kept:
        feats1[kept:table_rows, :] = jnp.zeros((table_rows - kept, features), jnp.bfloat16)
    emb = emb_ref[...].astype(jnp.float32)
    if kinds < 8:
        emb = jnp.concatenate([emb, jnp.zeros((8 - kinds, features), jnp.float32)], axis=0)
    emb = emb.astype(jnp.bfloat16)
    scales = [decay_ref[b] * (-LOG2E) for b in range(basis_count)]

    lane = lax.broadcasted_iota(jnp.int32, (8, LANES), 1)
    sub = lax.broadcasted_iota(jnp.int32, (8, LANES), 0)
    for copy in place_copies:
        copy.wait_recv()

    flat = [jnp.zeros((8, LANES), jnp.float32) for _ in range(tables)]
    for off in itertools.product((-1, 0, 1), repeat=3):
        source = tuple(canonical(d, n) for d, n in zip(off, sizes))
        cell = record[...] if source == (0, 0, 0) else places[code_of(source)]
        for component, delta in enumerate(off):
            if delta:
                cell = jnp.where(sub == component, cell + float(delta), cell)
        column = code_of(off) * slots
        tile, start = divmod(column + (shift_x if column >= lead else 0), LANES)
        if start:
            cell = pltpu.roll(cell, start, 1)
        stop = start + slots
        flat[tile] = jnp.where((lane >= start) & (lane < stop), cell, flat[tile])
        if stop > LANES:
            flat[tile + 1] = jnp.where(lane < stop - LANES, cell, flat[tile + 1])

    for tile in range(tiles):
        span = slice(tile * LANES, (tile + 1) * LANES)
        terms = []
        for part in (tile, tile + first) if merge and tile + first < tables else (tile,):
            r2 = jnp.zeros((slots, LANES), jnp.float32)
            for c in range(3):
                delta = flat[part][c : c + 1, :] - own_pos[c]
                r2 = r2 + delta * delta
            terms.append((r2, hist[pl.ds(part, slots, stride=hi_rows), :]))
        for b in range(basis_count):
            basis[b * slots : (b + 1) * slots, span] = sum(
                jnp.exp2(r2 * scales[b]) * times for r2, times in terms
            ).astype(jnp.bfloat16)
        one_hot = jnp.where(
            flat[tile][3:4, :].astype(jnp.int32) == sub, 1.0, 0.0
        )
        feats0[span, :] = jnp.dot(
            jnp.transpose(one_hot).astype(jnp.bfloat16), emb, preferred_element_type=jnp.float32
        ).astype(jnp.bfloat16)

    def interaction(layer, feats, hidden):
        collected = jnp.dot(basis[...], feats[...], preferred_element_type=jnp.float32)
        weight = radial_ref[layer].astype(jnp.float32)
        message = jnp.zeros((slots, features), jnp.float32)
        for b in range(basis_count):
            message = message + collected[b * slots : (b + 1) * slots] * weight[b : b + 1]
        inv_scale = lax.rsqrt(jnp.mean(message * message, axis=-1, keepdims=True) + 1e-05)
        normed = (message * inv_scale).astype(jnp.bfloat16)
        value = jnp.dot(normed, node_ref[layer], preferred_element_type=jnp.float32)
        update = value / (1.0 + jnp.exp(-value))
        return (hidden + update).astype(jnp.bfloat16)

    hidden1 = interaction(0, feats0, own_hidden)
    own_rows = pl.ds(code_of((0, 0, 0)) * slots, slots)
    feats1[own_rows, :] = hidden1

    def hidden_copy(off):
        code = code_of(off)
        return pltpu.make_async_remote_copy(
            src_ref=feats1.at[own_rows],
            dst_ref=feats1.at[pl.ds(code * slots, slots)],
            send_sem=hid_send.at[code],
            recv_sem=hid_recv.at[code],
            device_id=device(tuple(-d for d in off)),
            device_id_type=MESH,
        )

    hidden_copies = [hidden_copy(off) for off in neighbours]
    for copy in hidden_copies:
        copy.start()

    species_row = record[3:4, :]
    offsets = jnp.zeros((1, LANES), jnp.float32)
    for kind in range(kinds):
        offsets = jnp.where(species_row == float(kind), bias_ref[kind], offsets)
    offsets = jnp.where(lane[0:1] < slots, offsets, 0.0)

    for copy in hidden_copies:
        copy.wait_recv()
    for off in itertools.product((-1, 0, 1), repeat=3):
        source = tuple(canonical(d, n) for d, n in zip(off, sizes))
        if source != off and code_of(off) * slots < kept:
            feats1[pl.ds(code_of(off) * slots, slots), :] = feats1[
                pl.ds(code_of(source) * slots, slots), :
            ]
    hidden2 = interaction(1, feats1, hidden1.astype(jnp.float32))
    padded = jnp.concatenate(
        [hidden2, jnp.zeros((LANES - slots, features), jnp.bfloat16)], axis=0
    )
    readout = jnp.broadcast_to(readout_ref[...], (16, features))
    per_atom = lax.dot_general(
        readout, padded, (((1,), (1,)), ((), ())), preferred_element_type=jnp.float32
    )
    running = per_atom[0:1, :] + offsets
    out_ref[0:1, :] = running

    for axes, shifts, buf, send, recv in zip(
        stages, stage_shifts, stage_bufs, stage_sems[0::2], stage_sems[1::2]
    ):
        def rank_of(coords):
            rank = 0
            for name, coord, count in zip(AXES, coords, sizes):
                if name in axes:
                    rank = rank * count + coord
            return rank

        mine = rank_of(me)
        buf[mine] = running
        copies = []
        for index, shift in enumerate(shifts):
            copies.append(
                pltpu.make_async_remote_copy(
                    src_ref=buf.at[mine],
                    dst_ref=buf.at[mine],
                    send_sem=send.at[index],
                    recv_sem=recv.at[index],
                    device_id=device(shift),
                    device_id_type=MESH,
                )
            )
        for copy in copies:
            copy.start()
        for copy in copies:
            copy.wait_recv()
        running = jnp.sum(buf[...], axis=0)
        for copy in copies:
            copy.wait_send()
    out_ref[1:2, :] = jnp.broadcast_to(jnp.sum(running, axis=1, keepdims=True), (1, LANES))
    for copy in place_copies + hidden_copies:
        copy.wait_send()


def body(sizes, *args):
    positions, species, neighbours, _, embedding, decay, radial, _, readout, _ = args
    slots = positions.shape[-1]
    features = embedding.shape[1]
    basis_count = decay.shape[0]
    merge, lead, _, tables = fold_of(sizes, slots)
    tiles = pl.cdiv(lead if merge else 27 * slots, LANES)
    hi_rows = 16 * pl.cdiv(tables + 1, 16)
    devices = math.prod(sizes)
    stages = (AXES,) if devices <= 64 else tuple((name,) for name in AXES)
    stage_ranks = [
        math.prod(n for name, n in zip(AXES, sizes) if name in axes) for axes in stages
    ]
    vmem = pl.BlockSpec(memory_space=pltpu.VMEM)
    dma = pltpu.SemaphoreType.DMA
    scratch = [
        pltpu.VMEM((8, LANES), jnp.float32),
        pltpu.VMEM((27, 8, LANES), jnp.float32),
        pltpu.VMEM((slots * hi_rows, LANES), jnp.float32),
        pltpu.VMEM((slots, neighbours.shape[-1]), jnp.int32),
        pltpu.VMEM((basis_count * slots, tiles * LANES), jnp.bfloat16),
        pltpu.VMEM((tiles * LANES, features), jnp.bfloat16),
        pltpu.VMEM((tiles * LANES, features), jnp.bfloat16),
    ]
    scratch += [pltpu.VMEM((count, 1, LANES), jnp.float32) for count in stage_ranks]
    scratch += [dma((27,))] * 4
    for count in stage_ranks:
        scratch += [dma((max(count - 1, 1),))] * 2
    operands = (
        jnp.transpose(positions, (0, 1, 3, 2, 4)),
        *args[1:8],
        readout.reshape(1, features),
        args[9],
    )
    scratch[7:7] = [
        pltpu.SMEM(x.shape, x.dtype)
        if x.ndim == 1
        else pltpu.VMEM(x.shape, x.dtype)
        for x in operands
    ] + [dma((len(operands),))]
    out = pl.pallas_call(
        functools.partial(kernel, sizes, stages),
        out_shape=jax.ShapeDtypeStruct((2, LANES), jnp.float32),
        in_specs=[pl.BlockSpec(memory_space=pl.ANY)] * len(operands),
        out_specs=vmem,
        scratch_shapes=scratch,
        compiler_params=pltpu.CompilerParams(collective_id=0, has_side_effects=True),
    )(*operands)
    return out[0, :slots].reshape(species.shape), out[1, 0]


def solution(mesh):
    sizes = tuple(mesh.shape[name] for name in AXES)
    return jax.shard_map(
        functools.partial(body, sizes),
        mesh=mesh,
        in_specs=(
            P("gx", "gy", "gz", None, None),
            P("gx", "gy", "gz", None),
            P("gx", "gy", "gz", None, None),
            P("gx", "gy", "gz", None),
            P(),
            P(),
            P(),
            P(),
            P(),
            P(),
        ),
        out_specs=(P("gx", "gy", "gz", None), P()),
        check_vma=False,
    )
```

```python
import functools
import itertools
import math

import jax
import jax.numpy as jnp
from jax import lax
from jax.experimental import pallas as pl
from jax.experimental.pallas import tpu as pltpu
from jax.sharding import PartitionSpec as P

AXES = ("gx", "gy", "gz")
MESH = pl.DeviceIdType.MESH
LANES = 128
LOG2E = math.log2(math.e)


def distinct(count):
    return (0,) if count == 1 else (0, -1) if count == 2 else (0, -1, 1)


def canonical(offset, count):
    return 0 if count == 1 else -abs(offset) if count == 2 else offset


def code_of(offset):
    return 9 * (offset[0] + 1) + 3 * (offset[1] + 1) + offset[2] + 1


def fold_of(sizes, slots):
    merge = sizes[0] == 2
    lead = 18 * slots
    shift = -lead % LANES if merge else 0
    return merge, lead, shift, pl.cdiv(27 * slots + shift, LANES)


def kernel(
    sizes,
    stages,
    pos_any,
    spec_any,
    nbr_any,
    cnt_any,
    emb_any,
    decay_any,
    radial_any,
    node_any,
    readout_any,
    bias_any,
    out_ref,
    record,
    places,
    hist,
    codes,
    basis,
    feats0,
    feats1,
    *rest,
):
    anys = (
        pos_any, spec_any, nbr_any, cnt_any, emb_any, decay_any, radial_any, node_any, readout_any, bias_any,
    )
    pos_ref, spec_ref, nbr_ref, cnt_ref, emb_ref = rest[:5]
    decay_ref, radial_ref, node_ref, readout_ref, bias_ref = rest[5:10]
    load_sem = rest[10]
    loads = [
        pltpu.make_async_copy(src, dst, load_sem.at[n])
        for n, (src, dst) in enumerate(zip(anys, rest[:10]))
    ]
    rest = rest[11:]
    stage_bufs = rest[: len(stages)]
    pos_send, pos_recv, hid_send, hid_recv = rest[len(stages) : len(stages) + 4]
    stage_sems = rest[len(stages) + 4 :]
    me = tuple(lax.axis_index(name) for name in AXES)
    slots = pos_any.shape[-1]
    neighbour_count = nbr_any.shape[-1]
    features = emb_any.shape[1]
    kinds = emb_any.shape[0]
    basis_count = radial_ref.shape[1]
    layers = radial_ref.shape[0]
    tiles = basis.shape[1] // LANES
    merge, lead, shift_x, tables = fold_of(sizes, slots)
    first = (lead + shift_x) // LANES
    kept = lead if merge else 27 * slots
    hi_rows = hist.shape[0] // slots

    def device(shift):
        return tuple(
            lax.rem(coord + (delta % count), count) if delta % count else coord
            for coord, delta, count in zip(me, shift, sizes)
        )

    neighbours = [
        off for off in itertools.product(*(distinct(n) for n in sizes)) if off != (0, 0, 0)
    ]
    stage_shifts = [
        [
            shift
            for shift in itertools.product(
                *(range(n) if name in axes else (0,) for name, n in zip(AXES, sizes))
            )
            if any(shift)
        ]
        for axes in stages
    ]
    partners = {tuple((-d) % n for d, n in zip(off, sizes)) for off in neighbours}
    for shifts in stage_shifts:
        partners.update(shifts)
    barrier = pltpu.get_barrier_semaphore()
    for shift in sorted(partners):
        pl.semaphore_signal(barrier, inc=1, device_id=device(shift), device_id_type=MESH)

    for n in (0, 1, 3, 2, 4, 5, 6, 7, 8, 9):
        loads[n].start()
    for n in (0, 1, 3):
        loads[n].wait()
    record[...] = jnp.zeros(record.shape, jnp.float32)
    record[0:3, 0:slots] = pos_ref[0, 0, :, 0]
    record[3:4, 0:slots] = spec_ref[0, 0].astype(jnp.float32)
    counts = jnp.concatenate(
        [cnt_ref[0, 0].astype(jnp.float32), jnp.zeros((1, LANES - slots), jnp.float32)], axis=1
    )
    columns = jnp.transpose(
        jnp.concatenate([record[...], counts, jnp.zeros((3, LANES), jnp.float32)], axis=0)
    )[0:slots]
    own_pos = [
        jnp.broadcast_to(columns[:, c : c + 1], (slots, LANES)) for c in range(3)
    ]
    species_col = columns[:, 3:4]
    count_col = columns[:, 4:5]

    pl.semaphore_wait(barrier, len(partners))

    def place_copy(off):
        code = code_of(off)
        return pltpu.make_async_remote_copy(
            src_ref=record,
            dst_ref=places.at[code],
            send_sem=pos_send.at[code],
            recv_sem=pos_recv.at[code],
            device_id=device(tuple(-d for d in off)),
            device_id_type=MESH,
        )

    place_copies = [place_copy(off) for off in neighbours]
    for copy in place_copies:
        copy.start()

    loads[2].wait()
    raw = nbr_ref[0, 0, 0]
    live = lax.broadcasted_iota(jnp.int32, raw.shape, 1).astype(jnp.float32) < count_col
    raw = jnp.where(raw >= lead, raw + shift_x, raw)
    codes[...] = jnp.where(live, raw, hi_rows * LANES - 1)
    hi_iota = lax.broadcasted_iota(jnp.int32, (hi_rows, neighbour_count), 0)
    lo_iota = lax.broadcasted_iota(jnp.int32, (LANES, neighbour_count), 0)
    for atom in range(slots):
        row = codes[atom : atom + 1, :]
        high = jnp.where((row >> 7) == hi_iota, 1.0, 0.0).astype(jnp.bfloat16)
        low = jnp.where((row & (LANES - 1)) == lo_iota, 1.0, 0.0).astype(jnp.bfloat16)
        hist[atom * hi_rows : (atom + 1) * hi_rows, :] = lax.dot_general(
            high, low, (((1,), (1,)), ((), ())), preferred_element_type=jnp.float32
        )

    for n in range(4, 10):
        loads[n].wait()
    own_hidden = jnp.zeros((slots, features), jnp.float32)
    for kind in range(kinds):
        own_hidden = jnp.where(
            species_col == float(kind), emb_ref[kind : kind + 1, :].astype(jnp.float32), own_hidden
        )
    table_rows = feats1.shape[0]
    if table_rows > kept:
        feats1[kept:table_rows, :] = jnp.zeros((table_rows - kept, features), jnp.bfloat16)
    emb = emb_ref[...].astype(jnp.float32)
    if kinds < 8:
        emb = jnp.concatenate([emb, jnp.zeros((8 - kinds, features), jnp.float32)], axis=0)
    emb = emb.astype(jnp.bfloat16)
    scales = [decay_ref[b] * (-LOG2E) for b in range(basis_count)]

    lane = lax.broadcasted_iota(jnp.int32, (8, LANES), 1)
    sub = lax.broadcasted_iota(jnp.int32, (8, LANES), 0)
    for copy in place_copies:
        copy.wait_recv()

    flat = [jnp.zeros((4, LANES), jnp.float32) for _ in range(tables)]
    lane4 = lane[0:4]
    sub4 = sub[0:4]
    for off in itertools.product((-1, 0, 1), repeat=3):
        source = tuple(canonical(d, n) for d, n in zip(off, sizes))
        cell = record[...] if source == (0, 0, 0) else places[code_of(source)]
        for component, delta in enumerate(off):
            if delta:
                cell = jnp.where(sub4 == component, cell + float(delta), cell)
        column = code_of(off) * slots
        tile, start = divmod(column + (shift_x if column >= lead else 0), LANES)
        if start:
            cell = pltpu.roll(cell, start, 1)
        stop = start + slots
        flat[tile] = jnp.where((lane4 >= start) & (lane4 < stop), cell, flat[tile])
        if stop > LANES:
            flat[tile + 1] = jnp.where(lane4 < stop - LANES, cell, flat[tile + 1])

    for tile in range(tiles):
        span = slice(tile * LANES, (tile + 1) * LANES)
        terms = []
        for part in (tile, tile + first) if merge and tile + first < tables else (tile,):
            r2 = jnp.zeros((slots, LANES), jnp.float32)
            for c in range(3):
                delta = flat[part][c : c + 1, :] - own_pos[c]
                r2 = r2 + delta * delta
            terms.append((r2, hist[pl.ds(part, slots, stride=hi_rows), :]))
        for b in range(basis_count):
            basis[b * slots : (b + 1) * slots, span] = sum(
                jnp.exp2(r2 * scales[b]) * times for r2, times in terms
            ).astype(jnp.bfloat16)
        one_hot = jnp.where(
            flat[tile][3:4, :].astype(jnp.int32) == sub, 1.0, 0.0
        )
        feats0[span, :] = jnp.dot(
            jnp.transpose(one_hot).astype(jnp.bfloat16), emb, preferred_element_type=jnp.float32
        ).astype(jnp.bfloat16)

    def interaction(layer, feats, hidden):
        collected = jnp.dot(basis[...], feats[...], preferred_element_type=jnp.float32)
        weight = radial_ref[layer].astype(jnp.float32)
        message = jnp.zeros((slots, features), jnp.float32)
        for b in range(basis_count):
            message = message + collected[b * slots : (b + 1) * slots] * weight[b : b + 1]
        inv_scale = lax.rsqrt(jnp.mean(message * message, axis=-1, keepdims=True) + 1e-05)
        normed = (message * inv_scale).astype(jnp.bfloat16)
        value = jnp.dot(normed, node_ref[layer], preferred_element_type=jnp.float32)
        update = value / (1.0 + jnp.exp(-value))
        return (hidden + update).astype(jnp.bfloat16)

    hidden1 = interaction(0, feats0, own_hidden)
    own_rows = pl.ds(code_of((0, 0, 0)) * slots, slots)
    feats1[own_rows, :] = hidden1

    def hidden_copy(off):
        code = code_of(off)
        return pltpu.make_async_remote_copy(
            src_ref=feats1.at[own_rows],
            dst_ref=feats1.at[pl.ds(code * slots, slots)],
            send_sem=hid_send.at[code],
            recv_sem=hid_recv.at[code],
            device_id=device(tuple(-d for d in off)),
            device_id_type=MESH,
        )

    hidden_copies = [hidden_copy(off) for off in neighbours]
    for copy in hidden_copies:
        copy.start()

    species_row = record[3:4, :]
    offsets = jnp.zeros((1, LANES), jnp.float32)
    for kind in range(kinds):
        offsets = jnp.where(species_row == float(kind), bias_ref[kind], offsets)
    offsets = jnp.where(lane[0:1] < slots, offsets, 0.0)

    for copy in hidden_copies:
        copy.wait_recv()
    for off in itertools.product((-1, 0, 1), repeat=3):
        source = tuple(canonical(d, n) for d, n in zip(off, sizes))
        if source != off and code_of(off) * slots < kept:
            feats1[pl.ds(code_of(off) * slots, slots), :] = feats1[
                pl.ds(code_of(source) * slots, slots), :
            ]
    hidden2 = interaction(1, feats1, hidden1.astype(jnp.float32))
    padded = jnp.concatenate(
        [hidden2, jnp.zeros((LANES - slots, features), jnp.bfloat16)], axis=0
    )
    readout = jnp.broadcast_to(readout_ref[...], (16, features))
    per_atom = lax.dot_general(
        readout, padded, (((1,), (1,)), ((), ())), preferred_element_type=jnp.float32
    )
    running = per_atom[0:1, :] + offsets
    out_ref[0:1, :] = running

    for axes, shifts, buf, send, recv in zip(
        stages, stage_shifts, stage_bufs, stage_sems[0::2], stage_sems[1::2]
    ):
        def rank_of(coords):
            rank = 0
            for name, coord, count in zip(AXES, coords, sizes):
                if name in axes:
                    rank = rank * count + coord
            return rank

        mine = rank_of(me)
        buf[mine] = running
        copies = []
        for index, shift in enumerate(shifts):
            copies.append(
                pltpu.make_async_remote_copy(
                    src_ref=buf.at[mine],
                    dst_ref=buf.at[mine],
                    send_sem=send.at[index],
                    recv_sem=recv.at[index],
                    device_id=device(shift),
                    device_id_type=MESH,
                )
            )
        for copy in copies:
            copy.start()
        for copy in copies:
            copy.wait_recv()
        running = jnp.sum(buf[...], axis=0)
        for copy in copies:
            copy.wait_send()
    out_ref[1:2, :] = jnp.broadcast_to(jnp.sum(running, axis=1, keepdims=True), (1, LANES))
    for copy in place_copies + hidden_copies:
        copy.wait_send()


def body(sizes, *args):
    positions, species, neighbours, _, embedding, decay, radial, _, readout, _ = args
    slots = positions.shape[-1]
    features = embedding.shape[1]
    basis_count = decay.shape[0]
    merge, lead, _, tables = fold_of(sizes, slots)
    tiles = pl.cdiv(lead if merge else 27 * slots, LANES)
    hi_rows = 16 * pl.cdiv(tables + 1, 16)
    devices = math.prod(sizes)
    stages = (AXES,) if devices <= 64 else tuple((name,) for name in AXES)
    stage_ranks = [
        math.prod(n for name, n in zip(AXES, sizes) if name in axes) for axes in stages
    ]
    vmem = pl.BlockSpec(memory_space=pltpu.VMEM)
    dma = pltpu.SemaphoreType.DMA
    scratch = [
        pltpu.VMEM((4, LANES), jnp.float32),
        pltpu.VMEM((27, 4, LANES), jnp.float32),
        pltpu.VMEM((slots * hi_rows, LANES), jnp.float32),
        pltpu.VMEM((slots, neighbours.shape[-1]), jnp.int32),
        pltpu.VMEM((basis_count * slots, tiles * LANES), jnp.bfloat16),
        pltpu.VMEM((tiles * LANES, features), jnp.bfloat16),
        pltpu.VMEM((tiles * LANES, features), jnp.bfloat16),
    ]
    scratch += [pltpu.VMEM((count, 1, LANES), jnp.float32) for count in stage_ranks]
    scratch += [dma((27,))] * 4
    for count in stage_ranks:
        scratch += [dma((max(count - 1, 1),))] * 2
    operands = (
        jnp.transpose(positions, (0, 1, 3, 2, 4)),
        *args[1:8],
        readout.reshape(1, features),
        args[9],
    )
    scratch[7:7] = [
        pltpu.SMEM(x.shape, x.dtype)
        if x.ndim == 1
        else pltpu.VMEM(x.shape, x.dtype)
        for x in operands
    ] + [dma((len(operands),))]
    out = pl.pallas_call(
        functools.partial(kernel, sizes, stages),
        out_shape=pltpu.VMEM((2, LANES), jnp.float32),
        in_specs=[pl.BlockSpec(memory_space=pl.ANY)] * len(operands),
        out_specs=vmem,
        scratch_shapes=scratch,
        compiler_params=pltpu.CompilerParams(collective_id=0, has_side_effects=True),
    )(*operands)
    return out[0, :slots].reshape(species.shape), out[1, 0]


def solution(mesh):
    sizes = tuple(mesh.shape[name] for name in AXES)
    return jax.shard_map(
        functools.partial(body, sizes),
        mesh=mesh,
        in_specs=(
            P("gx", "gy", "gz", None, None),
            P("gx", "gy", "gz", None),
            P("gx", "gy", "gz", None, None),
            P("gx", "gy", "gz", None),
            P(),
            P(),
            P(),
            P(),
            P(),
            P(),
        ),
        out_specs=(P("gx", "gy", "gz", None), P()),
        check_vma=False,
    )
```

```python
import functools
import itertools
import math

import jax
import jax.numpy as jnp
from jax import lax
from jax.experimental import pallas as pl
from jax.experimental.pallas import tpu as pltpu
from jax.sharding import PartitionSpec as P

AXES = ("gx", "gy", "gz")
MESH = pl.DeviceIdType.MESH
LANES = 128
LOG2E = math.log2(math.e)


def distinct(count):
    return (0,) if count == 1 else (0, -1) if count == 2 else (0, -1, 1)


def canonical(offset, count):
    return 0 if count == 1 else -abs(offset) if count == 2 else offset


def code_of(offset):
    return 9 * (offset[0] + 1) + 3 * (offset[1] + 1) + offset[2] + 1


def fold_of(sizes, slots):
    merge = False
    lead = 18 * slots
    shift = -lead % LANES if merge else 0
    return merge, lead, shift, pl.cdiv(27 * slots + shift, LANES)


def kernel(
    sizes,
    stages,
    pos_any,
    spec_any,
    nbr_any,
    cnt_any,
    emb_any,
    decay_any,
    radial_any,
    node_any,
    readout_any,
    bias_any,
    out_ref,
    record,
    places,
    hist,
    codes,
    basis,
    feats0,
    feats1,
    *rest,
):
    anys = (
        pos_any, spec_any, nbr_any, cnt_any, emb_any, decay_any, radial_any, node_any, readout_any, bias_any,
    )
    pos_ref, spec_ref, nbr_ref, cnt_ref, emb_ref = rest[:5]
    decay_ref, radial_ref, node_ref, readout_ref, bias_ref = rest[5:10]
    load_sem = rest[10]
    loads = [
        pltpu.make_async_copy(src, dst, load_sem.at[n])
        for n, (src, dst) in enumerate(zip(anys, rest[:10]))
    ]
    rest = rest[11:]
    stage_bufs = rest[: len(stages)]
    pos_send, pos_recv, hid_send, hid_recv = rest[len(stages) : len(stages) + 4]
    stage_sems = rest[len(stages) + 4 :]
    me = tuple(lax.axis_index(name) for name in AXES)
    slots = pos_any.shape[-1]
    neighbour_count = nbr_any.shape[-1]
    features = emb_any.shape[1]
    kinds = emb_any.shape[0]
    basis_count = radial_ref.shape[1]
    layers = radial_ref.shape[0]
    tiles = basis.shape[1] // LANES
    merge, lead, shift_x, tables = fold_of(sizes, slots)
    first = (lead + shift_x) // LANES
    kept = lead if merge else 27 * slots
    hi_rows = hist.shape[0] // slots

    def device(shift):
        return tuple(
            lax.rem(coord + (delta % count), count) if delta % count else coord
            for coord, delta, count in zip(me, shift, sizes)
        )

    neighbours = [
        off for off in itertools.product(*(distinct(n) for n in sizes)) if off != (0, 0, 0)
    ]
    stage_shifts = [
        [
            shift
            for shift in itertools.product(
                *(range(n) if name in axes else (0,) for name, n in zip(AXES, sizes))
            )
            if any(shift)
        ]
        for axes in stages
    ]
    partners = {tuple((-d) % n for d, n in zip(off, sizes)) for off in neighbours}
    for shifts in stage_shifts:
        partners.update(shifts)
    barrier = pltpu.get_barrier_semaphore()
    for shift in sorted(partners):
        pl.semaphore_signal(barrier, inc=1, device_id=device(shift), device_id_type=MESH)

    for n in (0, 1, 3, 2, 4, 5, 6, 7, 8, 9):
        loads[n].start()
    for n in (0, 1, 3):
        loads[n].wait()
    record[...] = jnp.zeros(record.shape, jnp.float32)
    record[0:3, 0:slots] = pos_ref[0, 0, :, 0]
    record[3:4, 0:slots] = spec_ref[0, 0].astype(jnp.float32)
    counts = jnp.concatenate(
        [cnt_ref[0, 0].astype(jnp.float32), jnp.zeros((1, LANES - slots), jnp.float32)], axis=1
    )
    columns = jnp.transpose(
        jnp.concatenate([record[...], counts, jnp.zeros((3, LANES), jnp.float32)], axis=0)
    )[0:slots]
    own_pos = [
        jnp.broadcast_to(columns[:, c : c + 1], (slots, LANES)) for c in range(3)
    ]
    species_col = columns[:, 3:4]
    count_col = columns[:, 4:5]

    pl.semaphore_wait(barrier, len(partners))

    def place_copy(off):
        code = code_of(off)
        return pltpu.make_async_remote_copy(
            src_ref=record,
            dst_ref=places.at[code],
            send_sem=pos_send.at[code],
            recv_sem=pos_recv.at[code],
            device_id=device(tuple(-d for d in off)),
            device_id_type=MESH,
        )

    place_copies = [place_copy(off) for off in neighbours]
    for copy in place_copies:
        copy.start()

    loads[2].wait()
    raw = nbr_ref[0, 0, 0]
    live = lax.broadcasted_iota(jnp.int32, raw.shape, 1).astype(jnp.float32) < count_col
    raw = jnp.where(raw >= lead, raw + shift_x, raw)
    codes[...] = jnp.where(live, raw, hi_rows * LANES - 1)
    hi_iota = lax.broadcasted_iota(jnp.int32, (hi_rows, neighbour_count), 0)
    lo_iota = lax.broadcasted_iota(jnp.int32, (LANES, neighbour_count), 0)
    for atom in range(slots):
        row = codes[atom : atom + 1, :]
        high = jnp.where((row >> 7) == hi_iota, 1.0, 0.0).astype(jnp.bfloat16)
        low = jnp.where((row & (LANES - 1)) == lo_iota, 1.0, 0.0).astype(jnp.bfloat16)
        hist[atom * hi_rows : (atom + 1) * hi_rows, :] = lax.dot_general(
            high, low, (((1,), (1,)), ((), ())), preferred_element_type=jnp.float32
        )

    for n in range(4, 10):
        loads[n].wait()
    own_hidden = jnp.zeros((slots, features), jnp.float32)
    for kind in range(kinds):
        own_hidden = jnp.where(
            species_col == float(kind), emb_ref[kind : kind + 1, :].astype(jnp.float32), own_hidden
        )
    table_rows = feats1.shape[0]
    if table_rows > kept:
        feats1[kept:table_rows, :] = jnp.zeros((table_rows - kept, features), jnp.bfloat16)
    emb = emb_ref[...].astype(jnp.float32)
    if kinds < 8:
        emb = jnp.concatenate([emb, jnp.zeros((8 - kinds, features), jnp.float32)], axis=0)
    emb = emb.astype(jnp.bfloat16)
    scales = [decay_ref[b] * (-LOG2E) for b in range(basis_count)]

    lane = lax.broadcasted_iota(jnp.int32, (8, LANES), 1)
    sub = lax.broadcasted_iota(jnp.int32, (8, LANES), 0)
    for copy in place_copies:
        copy.wait_recv()

    flat = [jnp.zeros((4, LANES), jnp.float32) for _ in range(tables)]
    lane4 = lane[0:4]
    sub4 = sub[0:4]
    for off in itertools.product((-1, 0, 1), repeat=3):
        source = tuple(canonical(d, n) for d, n in zip(off, sizes))
        cell = record[...] if source == (0, 0, 0) else places[code_of(source)]
        for component, delta in enumerate(off):
            if delta:
                cell = jnp.where(sub4 == component, cell + float(delta), cell)
        column = code_of(off) * slots
        tile, start = divmod(column + (shift_x if column >= lead else 0), LANES)
        if start:
            cell = pltpu.roll(cell, start, 1)
        stop = start + slots
        flat[tile] = jnp.where((lane4 >= start) & (lane4 < stop), cell, flat[tile])
        if stop > LANES:
            flat[tile + 1] = jnp.where(lane4 < stop - LANES, cell, flat[tile + 1])

    for tile in range(tiles):
        span = slice(tile * LANES, (tile + 1) * LANES)
        terms = []
        for part in (tile, tile + first) if merge and tile + first < tables else (tile,):
            r2 = jnp.zeros((slots, LANES), jnp.float32)
            for c in range(3):
                delta = flat[part][c : c + 1, :] - own_pos[c]
                r2 = r2 + delta * delta
            terms.append((r2, hist[pl.ds(part, slots, stride=hi_rows), :]))
        for b in range(basis_count):
            basis[b * slots : (b + 1) * slots, span] = sum(
                jnp.exp2(r2 * scales[b]) * times for r2, times in terms
            ).astype(jnp.bfloat16)
        one_hot = jnp.where(
            flat[tile][3:4, :].astype(jnp.int32) == sub, 1.0, 0.0
        )
        feats0[span, :] = jnp.dot(
            jnp.transpose(one_hot).astype(jnp.bfloat16), emb, preferred_element_type=jnp.float32
        ).astype(jnp.bfloat16)

    def interaction(layer, feats, hidden):
        weight = radial_ref[layer].astype(jnp.float32)
        message = jnp.zeros((slots, features), jnp.float32)
        step = basis_count // 4
        for lead_b in range(0, basis_count, step):
            collected = jnp.dot(
                basis[lead_b * slots : (lead_b + step) * slots, :],
                feats[...],
                preferred_element_type=jnp.float32,
            )
            for b in range(step):
                message = message + (
                    collected[b * slots : (b + 1) * slots] * weight[lead_b + b : lead_b + b + 1]
                )
        inv_scale = lax.rsqrt(jnp.mean(message * message, axis=-1, keepdims=True) + 1e-05)
        normed = (message * inv_scale).astype(jnp.bfloat16)
        value = jnp.dot(normed, node_ref[layer], preferred_element_type=jnp.float32)
        update = value / (1.0 + jnp.exp(-value))
        return (hidden + update).astype(jnp.bfloat16)

    hidden1 = interaction(0, feats0, own_hidden)
    own_rows = pl.ds(code_of((0, 0, 0)) * slots, slots)
    feats1[own_rows, :] = hidden1

    def hidden_copy(off):
        code = code_of(off)
        return pltpu.make_async_remote_copy(
            src_ref=feats1.at[own_rows],
            dst_ref=feats1.at[pl.ds(code * slots, slots)],
            send_sem=hid_send.at[code],
            recv_sem=hid_recv.at[code],
            device_id=device(tuple(-d for d in off)),
            device_id_type=MESH,
        )

    hidden_copies = [hidden_copy(off) for off in neighbours]
    for copy in hidden_copies:
        copy.start()

    species_row = record[3:4, :]
    offsets = jnp.zeros((1, LANES), jnp.float32)
    for kind in range(kinds):
        offsets = jnp.where(species_row == float(kind), bias_ref[kind], offsets)
    offsets = jnp.where(lane[0:1] < slots, offsets, 0.0)

    for copy in hidden_copies:
        copy.wait_recv()
    for off in itertools.product((-1, 0, 1), repeat=3):
        source = tuple(canonical(d, n) for d, n in zip(off, sizes))
        if source != off and code_of(off) * slots < kept:
            feats1[pl.ds(code_of(off) * slots, slots), :] = feats1[
                pl.ds(code_of(source) * slots, slots), :
            ]
    hidden2 = interaction(1, feats1, hidden1.astype(jnp.float32))
    padded = jnp.concatenate(
        [hidden2, jnp.zeros((LANES - slots, features), jnp.bfloat16)], axis=0
    )
    readout = jnp.broadcast_to(readout_ref[...], (16, features))
    per_atom = lax.dot_general(
        readout, padded, (((1,), (1,)), ((), ())), preferred_element_type=jnp.float32
    )
    running = per_atom[0:1, :] + offsets
    out_ref[0:1, :] = running

    for axes, shifts, buf, send, recv in zip(
        stages, stage_shifts, stage_bufs, stage_sems[0::2], stage_sems[1::2]
    ):
        def rank_of(coords):
            rank = 0
            for name, coord, count in zip(AXES, coords, sizes):
                if name in axes:
                    rank = rank * count + coord
            return rank

        mine = rank_of(me)
        buf[mine] = running
        copies = []
        for index, shift in enumerate(shifts):
            copies.append(
                pltpu.make_async_remote_copy(
                    src_ref=buf.at[mine],
                    dst_ref=buf.at[mine],
                    send_sem=send.at[index],
                    recv_sem=recv.at[index],
                    device_id=device(shift),
                    device_id_type=MESH,
                )
            )
        for copy in copies:
            copy.start()
        for copy in copies:
            copy.wait_recv()
        running = jnp.sum(buf[...], axis=0)
        for copy in copies:
            copy.wait_send()
    out_ref[1:2, :] = jnp.broadcast_to(jnp.sum(running, axis=1, keepdims=True), (1, LANES))
    for copy in place_copies + hidden_copies:
        copy.wait_send()


def body(sizes, *args):
    positions, species, neighbours, _, embedding, decay, radial, _, readout, _ = args
    slots = positions.shape[-1]
    features = embedding.shape[1]
    basis_count = decay.shape[0]
    merge, lead, _, tables = fold_of(sizes, slots)
    tiles = pl.cdiv(lead if merge else 27 * slots, LANES)
    hi_rows = 16 * pl.cdiv(tables + 1, 16)
    devices = math.prod(sizes)
    stages = (AXES,) if devices <= 64 else tuple((name,) for name in AXES)
    stage_ranks = [
        math.prod(n for name, n in zip(AXES, sizes) if name in axes) for axes in stages
    ]
    vmem = pl.BlockSpec(memory_space=pltpu.VMEM)
    dma = pltpu.SemaphoreType.DMA
    scratch = [
        pltpu.VMEM((4, LANES), jnp.float32),
        pltpu.VMEM((27, 4, LANES), jnp.float32),
        pltpu.VMEM((slots * hi_rows, LANES), jnp.float32),
        pltpu.VMEM((slots, neighbours.shape[-1]), jnp.int32),
        pltpu.VMEM((basis_count * slots, tiles * LANES), jnp.bfloat16),
        pltpu.VMEM((tiles * LANES, features), jnp.bfloat16),
        pltpu.VMEM((tiles * LANES, features), jnp.bfloat16),
    ]
    scratch += [pltpu.VMEM((count, 1, LANES), jnp.float32) for count in stage_ranks]
    scratch += [dma((27,))] * 4
    for count in stage_ranks:
        scratch += [dma((max(count - 1, 1),))] * 2
    operands = (
        jnp.transpose(positions, (0, 1, 3, 2, 4)),
        *args[1:8],
        readout.reshape(1, features),
        args[9],
    )
    scratch[7:7] = [
        pltpu.SMEM(x.shape, x.dtype)
        if x.ndim == 1
        else pltpu.VMEM(x.shape, x.dtype)
        for x in operands
    ] + [dma((len(operands),))]
    out = pl.pallas_call(
        functools.partial(kernel, sizes, stages),
        out_shape=pltpu.VMEM((2, LANES), jnp.float32),
        in_specs=[pl.BlockSpec(memory_space=pl.ANY)] * len(operands),
        out_specs=vmem,
        scratch_shapes=scratch,
        compiler_params=pltpu.CompilerParams(collective_id=0, has_side_effects=True),
    )(*operands)
    return out[0, :slots].reshape(species.shape), out[1, 0]


def solution(mesh):
    sizes = tuple(mesh.shape[name] for name in AXES)
    return jax.shard_map(
        functools.partial(body, sizes),
        mesh=mesh,
        in_specs=(
            P("gx", "gy", "gz", None, None),
            P("gx", "gy", "gz", None),
            P("gx", "gy", "gz", None, None),
            P("gx", "gy", "gz", None),
            P(),
            P(),
            P(),
            P(),
            P(),
            P(),
        ),
        out_specs=(P("gx", "gy", "gz", None), P()),
        check_vma=False,
    )
```
